1024 devices in a mesh: row: 16 (over y, core), col: 64 (over z, x).
Axes of the slice: x: 8, y: 8, z: 8, core: 2. Of those that a mesh axis runs over, the one named last changes fastest.
Arguments:
- tokens: bfloat16 [320, 8192], P('col', 'row'), may hold values from -6 to 6
- grad_out: bfloat16 [320, 8192], P('col', 'row'), may hold values from -6 to 6
- gate_weight: bfloat16 [8192, 28672], P('row', 'col'), may hold values from -0.0625 to 0.0625
- up_weight: bfloat16 [8192, 28672], P('row', 'col'), may hold values from -0.0625 to 0.0625
- down_weight: bfloat16 [28672, 8192], P('col', 'row'), may hold values from -0.03125 to 0.03125
Outputs:
- grad_tokens: bfloat16 [320, 8192], P('col', 'row')
- grad_gate_weight: bfloat16 [8192, 28672], P('row', 'col')
- grad_up_weight: bfloat16 [8192, 28672], P('row', 'col')
- grad_down_weight: bfloat16 [28672, 8192], P('col', 'row')
The draws below stay inside these ranges and needn't reach their ends.
All inputs are finite; a program needn't handle non-finite values.
Results may differ from the reference program's by a relative error of at most 0.0049.
Values may be sent and summed in bfloat16 or wider, within the bound.
A program may use at most 32 MiB of HBM per device.

```python
import jax
import jax.numpy as jnp

D = 8192
FF = 28672
TOKENS = 320


def steps_of(stream_key, dims, shards, low, top_value):
    def one(axis_at, blocks):
        steps = jax.random.uniform(jax.random.fold_in(jax.random.fold_in(stream_key, 6), axis_at), (blocks,), jnp.float32, low / len(shards), top_value / len(shards))
        return jnp.repeat(jnp.exp(steps), dims[axis_at] // blocks).reshape((-1,) + (1,) * (len(dims) - axis_at - 1))

    factor_of = one(*shards[0])
    for cut in shards[1:]:
        factor_of = factor_of * one(*cut)
    return factor_of


def gaussian(key, shape, spread, reach, pieces=(), dtype=jnp.bfloat16):
    gain = steps_of(key, shape, pieces, -0.22, 0.18) if pieces else 1.0
    array = jax.random.normal(key, shape, jnp.float32) * spread * gain
    return jnp.minimum(jnp.maximum(array, -reach), reach).astype(dtype)


def setup_inputs(seed: int = 0) -> dict:
    seeds = jax.random.split(jax.random.key(seed), 6)
    tokens = gaussian(seeds[0], (TOKENS, D), 1.0, 6.0, ((0, 64), (1, 16)))
    grad_out = gaussian(seeds[1], (TOKENS, D), 1.0, 6.0, ((0, 64), (1, 16)))
    gate_weight = gaussian(seeds[2], (D, FF), D ** -0.5, 0.0625, ((0, 16), (1, 64)))
    up_weight = gaussian(seeds[3], (D, FF), D ** -0.5, 0.0625, ((0, 16), (1, 64)))
    down_weight = gaussian(seeds[4], (FF, D), FF ** -0.5, 0.03125, ((0, 64), (1, 16)))
    return dict(tokens=tokens, grad_out=grad_out, gate_weight=gate_weight, up_weight=up_weight, down_weight=down_weight)


def hidden_grads(gate_sum, up_sum, back_sum):
    sigmoid_gate = 1.0 / (1.0 + jnp.exp(-gate_sum))
    activated = gate_sum * sigmoid_gate
    hidden = (activated * up_sum).astype(jnp.bfloat16)
    grad_up = (back_sum * activated).astype(jnp.bfloat16)
    slope = sigmoid_gate * (1.0 + gate_sum * (1.0 - sigmoid_gate))
    grad_gate = (back_sum * up_sum * slope).astype(jnp.bfloat16)
    return hidden, grad_gate, grad_up


def reference(tokens, grad_out, gate_weight, up_weight, down_weight):
    gate_sum = jnp.dot(tokens, gate_weight, preferred_element_type=jnp.float32)
    up_sum = jnp.dot(tokens, up_weight, preferred_element_type=jnp.float32)
    back_sum = jnp.dot(grad_out, down_weight.T, preferred_element_type=jnp.float32)
    hidden, grad_gate, grad_up = hidden_grads(gate_sum, up_sum, back_sum)
    grad_down_weight = jnp.dot(hidden.T, grad_out, preferred_element_type=jnp.float32).astype(jnp.bfloat16)
    grad_gate_weight = jnp.dot(tokens.T, grad_gate, preferred_element_type=jnp.float32).astype(jnp.bfloat16)
    grad_up_weight = jnp.dot(tokens.T, grad_up, preferred_element_type=jnp.float32).astype(jnp.bfloat16)
    grad_tokens = jnp.dot(grad_gate, gate_weight.T, preferred_element_type=jnp.float32)
    grad_tokens = grad_tokens + jnp.dot(grad_up, up_weight.T, preferred_element_type=jnp.float32)
    return grad_tokens.astype(jnp.bfloat16), grad_gate_weight, grad_up_weight, grad_down_weight
```

```python
import functools

import jax
import jax.numpy as jnp
from jax import lax
from jax.experimental import pallas as pl
from jax.experimental.pallas import tpu as pltpu
from jax.sharding import PartitionSpec as P

MESH = pl.DeviceIdType.MESH
BF16 = jnp.bfloat16
F32 = jnp.float32
PAD = 8


def near_first(n):
    order = []
    for k in range(1, n // 2 + 1):
        order.append(k)
        if n - k != k:
            order.append(n - k)
    return order


def across(a, b):
    return lax.dot_general(a, b, (((1,), (1,)), ((), ())), preferred_element_type=F32)


def down(a, b):
    return lax.dot_general(a, b, (((0,), (0,)), ((), ())), preferred_element_type=F32)


def plain(a, b):
    return lax.dot_general(a, b, (((1,), (0,)), ((), ())), preferred_element_type=F32)


def kernel(
    n, nx,
    tok_ref, grad_ref, wg_ref, wu_ref, wd_ref,
    gtok_ref, gg_out, gu_out, gd_out,
    tok_in, grad_in, w_all, tok1, grad1, tok_full, grad_x, grad_full,
    pair_src, pair_dst, own_sum, y_src, y_dst,
    back, back_dst, own_back, yb_src, yb_dst,
    hid, d_dst, d_src, e_src, e_dst,
    load_sem, s_tok1, r_tok1, s_grad1, r_grad1, s_tok2, r_tok2, s_grad2, r_grad2,
    s_pair, r_pair, s_y, r_y, s_pairb, r_pairb, s_yb, r_yb, s_hid, r_hid, s_fwd, s_d, r_d, s_e, r_e,
):
    rows, width = tok_ref.shape
    group = rows * nx
    hidden = wd_ref.shape[0]
    two = 2 * hidden
    half = n // 2

    row, col = lax.axis_index("row"), lax.axis_index("col")
    y, core = lax.div(row, 2), lax.rem(row, 2)
    z, x = lax.div(col, nx), lax.rem(col, nx)
    other = row + 1 - 2 * core

    def at_x(k):
        return (row, z * nx + k)

    def at_z(k):
        return (row, k * nx + x)

    def at_y(k):
        return (2 * k + core, col)

    pair = (other, col)

    def send(src, dst, s, r, device):
        return pltpu.make_async_remote_copy(
            src_ref=src, dst_ref=dst, send_sem=s, recv_sem=r, device_id=device, device_id_type=MESH
        )

    def step(a, k, m):
        return lax.rem(a + k, m)

    def mine(g):
        k = lax.rem(z - g + n, n)
        return core == jnp.where((k >= 1) & (k <= half), 1, 0)

    def kept(m, who):
        k = who * (m + 1) + (1 - who) * ((n - m) % n)
        return lax.rem(z - k + 2 * n, n)

    loads = [
        pltpu.make_async_copy(wg_ref, w_all.at[pl.ds(0, hidden)], load_sem.at[0]),
        pltpu.make_async_copy(wu_ref, w_all.at[pl.ds(hidden, hidden)], load_sem.at[1]),
        pltpu.make_async_copy(wd_ref, w_all.at[pl.ds(two, hidden)], load_sem.at[2]),
    ]
    fetches = [
        pltpu.make_async_copy(tok_ref, tok_in, load_sem.at[3]),
        pltpu.make_async_copy(grad_ref, grad_in, load_sem.at[4]),
    ]
    for load in fetches + loads:
        load.start()

    barrier = pltpu.get_barrier_semaphore()
    peers = (
        [at_x(step(x, k, nx)) for k in range(1, nx)]
        + [at_z(step(z, k, n)) for k in range(1, n)]
        + [at_y(step(y, k, n)) for k in range(1, n)]
        + [pair]
    )
    for peer in peers:
        pl.semaphore_signal(barrier, inc=1, device_id=peer, device_id_type=MESH)

    blank = jnp.zeros((PAD - rows, width), BF16)
    for load in fetches:
        load.wait()
    tok1[x] = jnp.concatenate([tok_in[...], blank], axis=0)
    grad1[z] = jnp.concatenate([grad_in[...], blank], axis=0)

    def keep_matrix(blocks):
        shape = (rows * blocks, PAD * blocks)
        i = lax.broadcasted_iota(jnp.int32, shape, 0)
        j = lax.broadcasted_iota(jnp.int32, shape, 1)
        low = j & (PAD - 1)
        return ((low < rows) & (i == (j >> 3) * rows + low)).astype(F32).astype(BF16)

    pl.semaphore_wait(barrier, len(peers))

    sends = []
    for k in near_first(nx)[::-1]:
        copy = send(tok1.at[x], tok1.at[x], s_tok1.at[k], r_tok1.at[x], at_x(step(x, k, nx)))
        copy.start()
        sends.append(copy)
    for k in near_first(n)[::-1]:
        copy = send(grad1.at[z], grad1.at[z], s_grad1.at[k], r_grad1.at[z], at_z(step(z, k, n)))
        copy.start()
        sends.append(copy)

    def arrived(dst, sem, slot):
        send(dst.at[slot], dst.at[slot], sem.at[slot], sem.at[slot], pair).wait_recv()

    for k in range(1, nx):
        arrived(tok1, r_tok1, step(x, k, nx))
    tok_full[z] = plain(keep_matrix(nx), tok1[...].reshape(nx * PAD, width)).astype(BF16)
    for k in near_first(n):
        copy = send(tok_full.at[z], tok_full.at[z], s_tok2.at[k], r_tok2.at[z], at_z(step(z, k, n)))
        copy.start()
        sends.append(copy)
    for k in range(1, n):
        arrived(grad1, r_grad1, step(z, k, n))
    grad_x[x] = plain(keep_matrix(n), grad1[...].reshape(n * PAD, width)).astype(BF16)
    for k in near_first(nx):
        copy = send(grad_x.at[x], grad_x.at[x], s_grad2.at[k], r_grad2.at[x], at_x(step(x, k, nx)))
        copy.start()
        sends.append(copy)

    for load in loads:
        load.wait()

    def token_group(g):
        @pl.when(g != z)
        def _():
            arrived(tok_full, r_tok2, g)

        return across(tok_full[g], w_all[pl.ds(0, two), :])

    y_copies = []
    for m in range(half):
        g = kept(m, 1 - core)
        pair_src[m] = token_group(g)
        copy = send(pair_src.at[m], pair_dst.at[m], s_pair.at[m], r_pair.at[m], pair)
        copy.start()
        sends.append(copy)
        g = kept(m, core)
        part = token_group(g)
        copy.wait_recv()
        total = part + pair_dst[m]
        y_src[m] = total.astype(BF16)
        copy = send(y_src.at[m], y_dst.at[y], s_y.at[m], r_y.at[y], at_y(g))
        y_copies.append((g, copy))

        @pl.when(g != y)
        def _(copy=copy):
            copy.start()

        @pl.when(g == y)
        def _(total=total):
            own_sum[...] = total

    for k in range(1, nx):
        arrived(grad_x, r_grad2, step(x, k, nx))
    shape = (group * n, group * n)
    i = lax.broadcasted_iota(jnp.int32, shape, 0)
    j = lax.broadcasted_iota(jnp.int32, shape, 1)

    def split(v):
        block = lax.div(v, rows)
        return block >> (nx.bit_length() - 1), block & (nx - 1), v - block * rows

    zi, xi, ti = split(i)
    xj = lax.div(j, rows * n)
    zj = lax.div(j - xj * (rows * n), rows)
    tj = j - (xj * n + zj) * rows
    order = ((zi == zj) & (xi == xj) & (ti == tj)).astype(F32).astype(BF16)
    grad_full[...] = plain(order, grad_x[...].reshape(group * n, width)).astype(BF16)
    back[...] = across(grad_full[...], w_all[pl.ds(two, hidden), :]).reshape(n, group, hidden)

    b_copies = []
    for m in range(half):
        g = kept(m, 1 - core)
        copy = send(back.at[g], back_dst.at[m], s_pairb.at[m], r_pairb.at[m], pair)
        copy.start()
        b_copies.append(copy)
        sends.append(copy)
    yb_copies = []
    for m in range(half):
        g = kept(m, core)
        b_copies[m].wait_recv()
        total = back[g] + back_dst[m]
        yb_src[m] = total.astype(BF16)
        copy = send(yb_src.at[m], yb_dst.at[y], s_yb.at[m], r_yb.at[y], at_y(g))
        yb_copies.append((g, copy))

        @pl.when(g != y)
        def _(copy=copy):
            copy.start()

        @pl.when(g == y)
        def _(total=total):
            own_back[...] = total

    @pl.when(mine(y))
    def _():
        both = own_sum[...]
        for k in range(1, n):
            g = step(y, k, n)
            arrived(y_dst, r_y, g)
            both = both + y_dst[g].astype(F32)
        gate_sum, up_sum = both[:, :hidden], both[:, hidden:]
        back_sum = own_back[...]
        for k in range(1, n):
            g = step(y, k, n)
            arrived(yb_dst, r_yb, g)
            back_sum = back_sum + yb_dst[g].astype(F32)
        sigmoid_gate = 1.0 / (1.0 + jnp.exp(-gate_sum))
        activated = gate_sum * sigmoid_gate
        slope = sigmoid_gate * (1.0 + gate_sum * (1.0 - sigmoid_gate))
        grads = jnp.concatenate([back_sum * up_sum * slope, back_sum * activated], axis=1)
        hid[y, :, pl.ds(0, two)] = grads.astype(BF16)
        hid[y, :, pl.ds(two, hidden)] = (activated * up_sum).astype(BF16)
        for k in near_first(n):
            send(hid.at[y], hid.at[y], s_hid.at[k], r_hid.at[y], at_y(step(y, k, n))).start()

    d_copies = []
    for k in [0] + near_first(n):
        g = step(y, k, n)
        to_pair = send(hid.at[g], hid.at[g], s_fwd.at[k], r_hid.at[g], pair)
        if k == 0:

            @pl.when(jnp.logical_not(mine(g)))
            def _(g=g):
                arrived(hid, r_hid, g)
        else:
            arrived(hid, r_hid, g)

        @pl.when(mine(g))
        def _(to_pair=to_pair):
            to_pair.start()

        part = plain(hid[g, :, pl.ds(0, two)], w_all[pl.ds(0, two), :]).astype(BF16)
        copy = send(d_src.at[g], d_dst.at[z], s_d.at[k], r_d.at[z], at_z(g))
        d_copies.append((g, copy))

        @pl.when(g != z)
        def _(copy=copy, part=part, g=g):
            d_src[g] = part
            copy.start()

        @pl.when(g == z)
        def _(part=part):
            d_dst[z] = part

    tok_all = tok_full[...].reshape(n * group, width)
    grads_all = hid[:, :, pl.ds(0, two)].reshape(n * group, two)
    gg_out[...] = down(grads_all[:, :hidden], tok_all).astype(BF16)
    gu_out[...] = down(grads_all[:, hidden:], tok_all).astype(BF16)

    for k in range(1, n):
        arrived(d_dst, r_d, step(z, k, n))
    spread = keep_matrix(nx)
    spread = jnp.concatenate([spread] * n, axis=0)
    summed = down(spread, d_dst[...].reshape(n * group, width))
    e_src[...] = summed.reshape(nx, PAD, width)
    e_copies = []
    for k in near_first(nx)[::-1]:
        to = step(x, k, nx)
        copy = send(e_src.at[to], e_dst.at[x], s_e.at[k], r_e.at[x], at_x(to))
        copy.start()
        sends.append(copy)

    hidden_all = hid[:, :, pl.ds(two, hidden)].reshape(n * group, hidden)
    gd_out[...] = down(hidden_all, grad_full[...]).astype(BF16)

    total = e_src[x]
    for k in range(1, nx):
        g = step(x, k, nx)
        arrived(e_dst, r_e, g)
        total = total + e_dst[g]
    gtok_ref[...] = total[:rows].astype(BF16)

    for copy in sends:
        copy.wait_send()
    for target, copies in ((y, y_copies), (y, yb_copies), (z, d_copies)):
        for g, copy in copies:

            @pl.when(g != target)
            def _(copy=copy):
                copy.wait_send()

    @pl.when(mine(y))
    def _():
        for k in near_first(n):
            send(hid.at[y], hid.at[y], s_hid.at[k], r_hid.at[y], at_y(step(y, k, n))).wait_send()

    for k in range(n):
        g = step(y, k, n)

        @pl.when(mine(g))
        def _(g=g, k=k):
            send(hid.at[g], hid.at[g], s_fwd.at[k], r_hid.at[g], pair).wait_send()


def shards(n, nx, tokens, grad_out, gate_weight, up_weight, down_weight):
    rows, width = tokens.shape
    hidden = down_weight.shape[0]
    two, group, half = 2 * hidden, rows * nx, n // 2
    dma = pltpu.SemaphoreType.DMA
    out = jax.ShapeDtypeStruct((hidden, width), BF16)
    vmem = pl.BlockSpec(memory_space=pltpu.VMEM)
    hbm = pl.BlockSpec(memory_space=pl.ANY)
    grad_tokens, gate_t, up_t, grad_down = pl.pallas_call(
        functools.partial(kernel, n, nx),
        out_shape=(jax.ShapeDtypeStruct((rows, width), BF16), out, out, out),
        in_specs=[hbm] * 5,
        out_specs=(vmem,) * 4,
        scratch_shapes=[
            pltpu.VMEM((rows, width), BF16),
            pltpu.VMEM((rows, width), BF16),
            pltpu.VMEM((3 * hidden, width), BF16),
            pltpu.VMEM((nx, PAD, width), BF16),
            pltpu.VMEM((n, PAD, width), BF16),
            pltpu.VMEM((n, group, width), BF16),
            pltpu.VMEM((nx, group, width), BF16),
            pltpu.VMEM((n * group, width), BF16),
            pltpu.VMEM((half, group, two), F32),
            pltpu.VMEM((half, group, two), F32),
            pltpu.VMEM((group, two), F32),
            pltpu.VMEM((half, group, two), BF16),
            pltpu.VMEM((n, group, two), BF16),
            pltpu.VMEM((n, group, hidden), F32),
            pltpu.VMEM((half, group, hidden), F32),
            pltpu.VMEM((group, hidden), F32),
            pltpu.VMEM((half, group, hidden), BF16),
            pltpu.VMEM((n, group, hidden), BF16),
            pltpu.VMEM((n, group, 3 * hidden), BF16),
            pltpu.VMEM((n, group, width), BF16),
            pltpu.VMEM((n, group, width), BF16),
            pltpu.VMEM((nx, PAD, width), F32),
            pltpu.VMEM((nx, PAD, width), F32),
            dma((5,)),
            dma((nx,)), dma((nx,)), dma((n,)), dma((n,)), dma((n,)), dma((n,)), dma((nx,)), dma((nx,)),
            dma((half,)), dma((half,)), dma((half,)), dma((n,)), dma((half,)), dma((half,)), dma((half,)), dma((n,)),
            dma((n,)), dma((n,)), dma((n,)), dma((n,)), dma((n,)), dma((nx,)), dma((nx,)),
        ],
        compiler_params=pltpu.CompilerParams(
            collective_id=0, has_side_effects=True, vmem_limit_bytes=67043328
        ),
        name="block",
    )(tokens, grad_out, gate_weight.T, up_weight.T, down_weight)
    return grad_tokens, gate_t.T, up_t.T, grad_down


def solution(mesh):
    n = mesh.shape["row"] // 2
    nx = mesh.shape["col"] // n
    placed = (P("col", "row"), P("col", "row"), P("row", "col"), P("row", "col"), P("col", "row"))
    return jax.shard_map(
        functools.partial(shards, n, nx),
        mesh=mesh,
        in_specs=placed,
        out_specs=(P("col", "row"), P("row", "col"), P("row", "col"), P("col", "row")),
        check_vma=False,
    )
```

```python
import functools

import jax
import jax.numpy as jnp
from jax import lax
from jax.experimental import pallas as pl
from jax.experimental.pallas import tpu as pltpu
from jax.sharding import PartitionSpec as P

MESH = pl.DeviceIdType.MESH
BF16 = jnp.bfloat16
F32 = jnp.float32
PAD = 8
LANES = 128
MIB = 1024 * 1024


def near_first(n):
    order = []
    for k in range(1, n // 2 + 1):
        order.append(k)
        if n - k != k:
            order.append(n - k)
    return order


def spaced(n, odd):
    return [0] * (1 - odd) + [k for k in near_first(n) if k % 2 == odd]


def groups_of(n):
    half = n // 2
    ks = ([(n - m) % n for m in range(half)], [m + 1 for m in range(half)])
    if n == 8:
        owners = ([0, 4, 1, 5], [2, 6, 3, 7])
    else:
        owners = (list(range(half)), list(range(half, n)))
    return ks, owners


def across(a, b):
    return lax.dot_general(a, b, (((1,), (1,)), ((), ())), preferred_element_type=F32)


def down(a, b):
    return lax.dot_general(a, b, (((0,), (0,)), ((), ())), preferred_element_type=F32)


def plain(a, b):
    return lax.dot_general(a, b, (((1,), (0,)), ((), ())), preferred_element_type=F32)


def iota(shape, dim):
    return lax.broadcasted_iota(jnp.int32, shape, dim)


def ones_where(mask):
    return mask.astype(F32).astype(BF16)


def kernel(
    n,
    tok_ref, grad_ref, wg_ref, wu_ref, wd_ref,
    gtok_ref, gg_out, gu_out, gd_out,
    tok_in, grad_in, packed, w_all, blocks, tok_full, grad_full,
    pair_src, pair_dst, own_sum, y_src, y_dst, hid_g, hid_h, d_src, d_dst, e_src, e_dst,
    load_sem, s_own, s_blk, r_blk, s_pair, r_pair, s_y, r_y, s_hid, r_hid, s_fwd, s_hidh, r_hidh, s_fwdh, s_d, r_d, s_e, r_e,
):
    rows, width = tok_in.shape
    hidden = wd_ref.shape[0]
    two = 2 * hidden
    half = n // 2
    side = rows * half
    group = 2 * side
    room = d_src.shape[2]
    parts = 2 * width // LANES
    block = rows * parts

    row, col = lax.axis_index("row"), lax.axis_index("col")
    y, core = lax.div(row, 2), lax.rem(row, 2)
    z, x = lax.div(col, n), lax.rem(col, n)
    odd = lax.rem(z + x, 2)
    pair = (row + 1 - 2 * core, col)
    spot = x + odd * (z - x)
    here = lax.div(spot, 2)

    def step(a, k):
        return lax.rem(a + k, n)

    def at_x(k):
        return (row, z * n + k)

    def at_z(k):
        return (row, k * n + x)

    def at_y(k):
        return (2 * k + core, col)

    def at_own(k):
        other = step(spot, k)
        return (row, (z * n + other) * (1 - odd) + (other * n + x) * odd)

    def send(src, dst, s, r, device):
        return pltpu.make_async_remote_copy(
            src_ref=src, dst_ref=dst, send_sem=s, recv_sem=r, device_id=device, device_id_type=MESH
        )

    def arrived(dst, sem):
        send(dst, dst, sem, sem, pair).wait_recv()

    ks, owners = groups_of(n)

    def pick(first, second, who):
        return first * (1 - who) + second * who

    def kept(m, who):
        return pick(ks[0][m], ks[1][m], who), pick(owners[0][m], owners[1][m], who)

    def mine(o):
        found = [o == pick(owners[0][m], owners[1][m], core) for m in range(half)]
        return functools.reduce(jnp.logical_or, found)

    def distance(o):
        return sum(jnp.where(o == owners[w][m], ks[w][m], 0) for w in range(2) for m in range(half))

    sends = []
    y_copies, d_copies, e_copies = [], [], []

    def drain():
        for copy in sends:
            copy.wait_send()
        for clash, copy in y_copies + d_copies + e_copies:

            @pl.when(jnp.logical_not(clash))
            def _(copy=copy):
                copy.wait_send()

    fetches = [
        pltpu.make_async_copy(tok_ref, tok_in, load_sem.at[0]),
        pltpu.make_async_copy(grad_ref, grad_in, load_sem.at[1]),
    ]
    loads = [
        pltpu.make_async_copy(wg_ref, w_all.at[pl.ds(0, hidden)], load_sem.at[2]),
        pltpu.make_async_copy(wu_ref, w_all.at[pl.ds(hidden, hidden)], load_sem.at[3]),
        pltpu.make_async_copy(wd_ref, w_all.at[pl.ds(two, hidden)], load_sem.at[4]),
    ]
    for load in fetches + loads:
        load.start()

    barrier = pltpu.get_barrier_semaphore()
    peers = [at(step(a, k)) for at, a in ((at_x, x), (at_z, z), (at_y, y)) for k in range(1, n)] + [pair]
    for peer in peers:
        pl.semaphore_signal(barrier, inc=1, device_id=peer, device_id_type=MESH)

    for load in fetches:
        load.wait()
    for a, ref in enumerate((tok_in, grad_in)):
        value = ref[...].astype(F32)
        for q in range(parts // 2):
            at = (a * (parts // 2) + q) * rows
            packed[pl.ds(at, rows), :] = value[:, q * LANES : (q + 1) * LANES]
    blocks[odd, 0, here] = packed[...].astype(BF16)

    total_rows = n * block
    v = iota((1, total_rows), 1)
    b = lax.div(v, block)
    q = lax.div(v - b * block, rows)
    to = q * (n * rows) + b * rows + (v - b * block - q * rows)
    regroup = ones_where(iota((total_rows, total_rows), 0) == to)

    pl.semaphore_wait(barrier, len(peers))

    own = blocks.at[odd, 0, here]
    for k in near_first(n)[::-1]:
        copy = send(own, own, s_own.at[k], r_blk.at[odd, 0, here], at_own(k))
        copy.start()
        sends.append(copy)
    same, differ = spaced(n, 0), spaced(n, 1)
    for s in range(half):
        for axis in range(2):
            is_own = odd == axis
            offset = jnp.where(is_own, same[s], differ[s])
            place = lax.div(step(z if axis else x, offset), 2)
            if s == 0:

                @pl.when(jnp.logical_not(is_own))
                def _(axis=axis, place=place):
                    arrived(blocks.at[axis, 0, place], r_blk.at[axis, 0, place])
            else:
                arrived(blocks.at[axis, 0, place], r_blk.at[axis, 0, place])
            for k in near_first(n):
                device = at_x(step(x, k)) if axis else at_z(step(z, k))
                copy = send(
                    blocks.at[axis, 0, place], blocks.at[axis, k, place],
                    s_blk.at[axis, k, s], r_blk.at[axis, k, place], device,
                )
                copy.start()
                sends.append(copy)

    for load in loads:
        load.wait()

    def partial(pairs):
        for k, _ in pairs:

            @pl.when(k != 0)
            def _(k=k):
                for axis in range(2):
                    for i in range(half):
                        arrived(blocks.at[axis, k, i], r_blk.at[axis, k, i])

        held = [
            jnp.concatenate([blocks[axis, k].reshape(half * block, LANES) for axis in range(2)], axis=0)
            for k, _ in pairs
        ]
        rows_of = plain(regroup, jnp.concatenate(held, axis=1)).astype(BF16)
        toks, grads = [], []
        for at, (_, o) in enumerate(pairs):
            lanes = rows_of[:, at * LANES : (at + 1) * LANES]
            cut = [lanes[q * group : (q + 1) * group] for q in range(parts)]
            toks.append(jnp.concatenate(cut[: parts // 2], axis=1))
            grads.append(jnp.concatenate(cut[parts // 2 :], axis=1))
            tok_full[o] = toks[-1]
            grad_full[o] = grads[-1]
        sums = across(jnp.concatenate(toks, axis=0), w_all[pl.ds(0, two), :])
        backs = across(jnp.concatenate(grads, axis=0), w_all[pl.ds(two, hidden), :])
        return jnp.concatenate([sums, backs], axis=1)

    batch = max(half // 2, 1)
    for m in range(0, half, batch):
        spots = range(m, m + batch)
        pair_src[m // batch] = partial([kept(i, 1 - core) for i in spots])
        copy = send(pair_src.at[m // batch], pair_dst.at[m // batch], s_pair.at[m], r_pair.at[m], pair)
        copy.start()
        sends.append(copy)
        part = partial([kept(i, core) for i in spots])
        copy.wait_recv()
        sums = part + pair_dst[m // batch]
        for at, i in enumerate(spots):
            _, g = kept(i, core)
            total = sums[at * group : (at + 1) * group]
            y_src[i] = total.astype(BF16)
            copy = send(y_src.at[i], y_dst.at[y], s_y.at[i], r_y.at[y], at_y(g))
            y_copies.append((g == y, copy))

            @pl.when(g != y)
            def _(copy=copy):
                copy.start()

            @pl.when(g == y)
            def _(total=total):
                own_sum[...] = total

    hid_order = near_first(n)
    direct = hid_order

    def handed_drain(lists):
        for ref, s_out, s_pass, r in lists:

            @pl.when(mine(y))
            def _(ref=ref, s_out=s_out, r=r):
                for copy in from_owner(ref, s_out, r):
                    copy.wait_send()

            for k in range(n):
                copy = to_pair(ref, s_pass, r, k)
                pl.when(mine(step(y, k)))(copy.wait_send)

    def from_owner(ref, s, r):
        return [send(ref.at[y], ref.at[y], s.at[k], r.at[y], at_y(step(y, k))) for k in direct]

    def to_pair(ref, s, r, k):
        g = step(y, k)
        return send(ref.at[g], ref.at[g], s.at[k], r.at[g], pair)

    def hand_on(ref, s, r, k):
        g = step(y, k)
        if k == 0:
            pl.when(jnp.logical_not(mine(g)))(lambda: arrived(ref.at[g], r.at[g]))
        else:
            arrived(ref.at[g], r.at[g])
        pl.when(mine(g))(lambda: to_pair(ref, s, r, k).start())

    @pl.when(mine(y))
    def _():
        all_sums = own_sum[...]
        for k in hid_order:
            g = step(y, k)
            arrived(y_dst.at[g], r_y.at[g])
            all_sums = all_sums + y_dst[g].astype(F32)
        gate_sum, up_sum, back_sum = all_sums[:, :hidden], all_sums[:, hidden:two], all_sums[:, two:]
        sigmoid_gate = 1.0 / (1.0 + jnp.exp(-gate_sum))
        activated = gate_sum * sigmoid_gate
        slope = sigmoid_gate * (1.0 + gate_sum * (1.0 - sigmoid_gate))
        grads = jnp.concatenate([back_sum * up_sum * slope, back_sum * activated], axis=1)
        hid_g[y] = grads.astype(BF16)
        for copy in from_owner(hid_g, s_hid, r_hid):
            copy.start()
        hid_h[y] = (activated * up_sum).astype(BF16)
        for copy in from_owner(hid_h, s_hidh, r_hidh):
            copy.start()

    def apart_for(count):
        i, j = iota((2 * room * count, 1), 0), iota((1, group * count), 1)
        block_of = lax.div(j, side)
        return ones_where(i == block_of * room + j - block_of * side)

    offsets = [0] + hid_order
    middle = n // 2 + 1
    for near in (offsets[:middle], offsets[middle:]):
        for k in near:
            hand_on(hid_g, s_fwd, r_hid, k)
        if not near:
            continue
        grads = jnp.concatenate([hid_g[step(y, k)] for k in near], axis=0)
        part = plain(grads, w_all[pl.ds(0, two), :]).astype(BF16)
        part = plain(apart_for(len(near)), part).astype(BF16)
        for at, k in enumerate(near):
            g = distance(step(y, k))
            home = g == 0
            for axis, a, place in ((0, z, at_z), (1, x, at_x)):
                device = place(step(a, n - g))
                first = (2 * at + axis) * room
                piece = part[first : first + room]
                d_src[axis, g] = piece
                copy = send(d_src.at[axis, g], d_dst.at[axis, g], s_d.at[axis, g], r_d.at[axis, g], device)
                d_copies.append((home, copy))

                @pl.when(jnp.logical_not(home))
                def _(copy=copy):
                    copy.start()

                @pl.when(home)
                def _(axis=axis, piece=piece):
                    d_dst[axis, 0] = piece

    for k in offsets:
        hand_on(hid_h, s_fwdh, r_hidh, k)

    tok_all = tok_full[...].reshape(n * group, width)
    grads_all = hid_g[...].reshape(n * group, two)
    gg_out[...] = down(grads_all[:, :hidden], tok_all).astype(BF16)
    gu_out[...] = down(grads_all[:, hidden:], tok_all).astype(BF16)

    i, j = iota((half * PAD, room), 0), iota((half * PAD, room), 1)
    low = i & (PAD - 1)
    spread = ones_where((low < rows) & (j == (i >> 3) * rows + low))
    spread = jnp.concatenate([spread] * n, axis=1)
    for axis in range(2):
        for k in range(1, n):
            arrived(d_dst.at[axis, k], r_d.at[axis, k])
        summed = plain(spread, d_dst[axis].reshape(n * room, width))
        e_src[axis] = summed.reshape(half, PAD, width)
        line, cross = (z, x) if axis else (x, z)
        for i in range(half):
            place = 2 * i + lax.rem(cross + axis, 2)
            device = at_z(place) if axis else at_x(place)
            is_self = place == line
            copy = send(e_src.at[axis, i], e_dst.at[line], s_e.at[axis, i], r_e.at[line], device)
            e_copies.append((is_self, copy))

            @pl.when(jnp.logical_not(is_self))
            def _(copy=copy):
                copy.start()

            @pl.when(is_self)
            def _(axis=axis, i=i, line=line):
                e_dst[line] = e_src[axis, i]

    grad_all = grad_full[...].reshape(n * group, width)
    hidden_all = hid_h[...].reshape(n * group, hidden)
    gd_out[...] = down(hidden_all, grad_all).astype(BF16)

    for k in range(1, n):
        g = step(spot, k)
        arrived(e_dst.at[g], r_e.at[g])
    gtok_ref[...] = jnp.sum(e_dst[...], axis=0)[:rows].astype(BF16)

    drain()
    handed_drain(((hid_g, s_hid, s_fwd, r_hid), (hid_h, s_hidh, s_fwdh, r_hidh)))


def put_out(*refs):
    count = (len(refs) - 1) // 2
    copies = [pltpu.make_async_copy(refs[i], refs[count + i], refs[-1].at[i]) for i in range(count)]
    for copy in copies:
        copy.start()
    for copy in copies:
        copy.wait()


def shards(n, tokens, grad_out, gate_weight, up_weight, down_weight):
    rows, width = tokens.shape
    hidden = down_weight.shape[0]
    two, half = 2 * hidden, n // 2
    side = rows * half
    batch = max(half // 2, 1)
    group = 2 * side
    room = -(-side // PAD) * PAD
    block = rows * 2 * width // LANES
    dma = pltpu.SemaphoreType.DMA
    out = jax.ShapeDtypeStruct((hidden, width), BF16)
    outs = (jax.ShapeDtypeStruct((rows, width), BF16), out, out, out)
    vmem = pl.BlockSpec(memory_space=pltpu.VMEM)
    hbm = pl.BlockSpec(memory_space=pltpu.HBM)
    results = pl.pallas_call(
        functools.partial(kernel, n),
        out_shape=outs,
        in_specs=[hbm] * 5,
        out_specs=(vmem,) * 4,
        scratch_shapes=[
            pltpu.VMEM((rows, width), BF16),
            pltpu.VMEM((rows, width), BF16),
            pltpu.VMEM((block, LANES), F32),
            pltpu.VMEM((3 * hidden, width), BF16),
            pltpu.VMEM((2, n, half, block, LANES), BF16),
            pltpu.VMEM((n, group, width), BF16),
            pltpu.VMEM((n, group, width), BF16),
            pltpu.VMEM((half // batch, batch * group, 3 * hidden), F32),
            pltpu.VMEM((half // batch, batch * group, 3 * hidden), F32),
            pltpu.VMEM((group, 3 * hidden), F32),
            pltpu.VMEM((half, group, 3 * hidden), BF16),
            pltpu.VMEM((n, group, 3 * hidden), BF16),
            pltpu.VMEM((n, group, two), BF16),
            pltpu.VMEM((n, group, hidden), BF16),
            pltpu.VMEM((2, n, room, width), BF16),
            pltpu.VMEM((2, n, room, width), BF16),
            pltpu.VMEM((2, half, PAD, width), F32),
            pltpu.VMEM((n, PAD, width), F32),
            dma((5,)),
            dma((n,)), dma((2, n, half)), dma((2, n, half)),
            dma((half,)), dma((half,)), dma((half,)), dma((n,)),
            dma((n,)), dma((n,)), dma((n,)), dma((n,)), dma((n,)), dma((n,)),
            dma((2, n)), dma((2, n)), dma((2, half)), dma((n,)),
        ],
        compiler_params=pltpu.CompilerParams(collective_id=0, has_side_effects=True, vmem_limit_bytes=32 * MIB),
        name="block",
    )(*[pltpu.with_memory_space_constraint(v, pltpu.HBM) for v in (tokens, grad_out, gate_weight.T, up_weight.T, down_weight)])
    grad_tokens, gate_t, up_t, grad_down = pl.pallas_call(
        put_out,
        out_shape=outs,
        in_specs=[vmem] * 4,
        out_specs=(hbm,) * 4,
        scratch_shapes=[dma((4,))],
        compiler_params=pltpu.CompilerParams(vmem_limit_bytes=16 * MIB),
        name="put_out",
    )(*results)
    return grad_tokens, gate_t.T, up_t.T, grad_down


def solution(mesh):
    n = mesh.shape["row"] // 2
    placed = (P("col", "row"), P("col", "row"), P("row", "col"), P("row", "col"), P("col", "row"))
    return jax.shard_map(
        functools.partial(shards, n),
        mesh=mesh,
        in_specs=placed,
        out_specs=(P("col", "row"), P("row", "col"), P("row", "col"), P("col", "row")),
        check_vma=False,
    )
```

```python
import functools

import jax
import jax.numpy as jnp
from jax import lax
from jax.experimental import pallas as pl
from jax.experimental.pallas import tpu as pltpu
from jax.sharding import PartitionSpec as P

MESH = pl.DeviceIdType.MESH
BF16 = jnp.bfloat16
F32 = jnp.float32
PAD = 8
LANES = 128
MIB = 1024 * 1024


def near_first(n):
    order = []
    for k in range(1, n // 2 + 1):
        order.append(k)
        if n - k != k:
            order.append(n - k)
    return order


def spaced(n, odd):
    return [0] * (1 - odd) + [k for k in near_first(n) if k % 2 == odd]


def groups_of(n):
    half = n // 2
    ks = ([(n - m) % n for m in range(half)], [m + 1 for m in range(half)])
    if n == 8:
        owners = ([0, 4, 1, 5], [2, 6, 3, 7])
    else:
        owners = (list(range(half)), list(range(half, n)))
    return ks, owners


def down(a, b):
    return lax.dot_general(a, b, (((0,), (0,)), ((), ())), preferred_element_type=F32)


def plain(a, b):
    return lax.dot_general(a, b, (((1,), (0,)), ((), ())), preferred_element_type=F32)


def iota(shape, dim):
    return lax.broadcasted_iota(jnp.int32, shape, dim)


def ones_where(mask):
    return mask.astype(F32).astype(BF16)


def kernel(
    n,
    tok_ref, grad_ref, wg_ref, wu_ref, wd_ref,
    gtok_ref, gg_out, gu_out, gd_out,
    tok_in, grad_in, packed, w_all, w_turned, blocks, tok_full, grad_full,
    pair_src, pair_dst, own_sum, y_src, y_dst, hid_g, hid_h, d_src, d_dst, e_src, e_dst,
    load_sem, s_own, s_blk, r_blk, s_pair, r_pair, s_y, r_y, s_hid, r_hid, s_fwd, s_hidh, r_hidh, s_fwdh, s_d, r_d, s_e, r_e,
):
    rows, width = tok_in.shape
    hidden = wd_ref.shape[0]
    two = 2 * hidden
    half = n // 2
    side = rows * half
    group = 2 * side
    room = d_src.shape[2]
    parts = 2 * width // LANES
    block = rows * parts

    row, col = lax.axis_index("row"), lax.axis_index("col")
    y, core = lax.div(row, 2), lax.rem(row, 2)
    z, x = lax.div(col, n), lax.rem(col, n)
    odd = lax.rem(z + x, 2)
    pair = (row + 1 - 2 * core, col)
    spot = x + odd * (z - x)
    here = lax.div(spot, 2)

    def step(a, k):
        return lax.rem(a + k, n)

    def at_x(k):
        return (row, z * n + k)

    def at_z(k):
        return (row, k * n + x)

    def at_y(k):
        return (2 * k + core, col)

    def at_own(k):
        other = step(spot, k)
        return (row, (z * n + other) * (1 - odd) + (other * n + x) * odd)

    def at_cross(k):
        return (row, (z * n + step(x, k)) * odd + (step(z, k) * n + x) * (1 - odd))

    def send(src, dst, s, r, device):
        return pltpu.make_async_remote_copy(
            src_ref=src, dst_ref=dst, send_sem=s, recv_sem=r, device_id=device, device_id_type=MESH
        )

    def arrived(dst, sem):
        send(dst, dst, sem, sem, pair).wait_recv()

    ks, owners = groups_of(n)

    def pick(first, second, who):
        return first * (1 - who) + second * who

    def kept(m, who):
        return pick(ks[0][m], ks[1][m], who), pick(owners[0][m], owners[1][m], who)

    def mine(o):
        found = [o == pick(owners[0][m], owners[1][m], core) for m in range(half)]
        return functools.reduce(jnp.logical_or, found)

    def distance(o):
        return sum(jnp.where(o == owners[w][m], ks[w][m], 0) for w in range(2) for m in range(half))

    sends = []
    y_copies, d_copies, e_copies = [], [], []

    def drain():
        for copy in sends:
            copy.wait_send()
        for clash, copy in y_copies + d_copies + e_copies:

            @pl.when(jnp.logical_not(clash))
            def _(copy=copy):
                copy.wait_send()

    fetches = [
        pltpu.make_async_copy(tok_ref, tok_in, load_sem.at[0]),
        pltpu.make_async_copy(grad_ref, grad_in, load_sem.at[1]),
    ]
    loads = [
        pltpu.make_async_copy(wg_ref, w_all.at[pl.ds(0, hidden)], load_sem.at[2]),
        pltpu.make_async_copy(wu_ref, w_all.at[pl.ds(hidden, hidden)], load_sem.at[3]),
        pltpu.make_async_copy(wd_ref, w_all.at[pl.ds(two, hidden)], load_sem.at[4]),
    ]
    for load in fetches + loads:
        load.start()

    barrier = pltpu.get_barrier_semaphore()
    peers = [at(step(a, k)) for at, a in ((at_x, x), (at_z, z), (at_y, y)) for k in range(1, n)] + [pair]
    for peer in peers:
        pl.semaphore_signal(barrier, inc=1, device_id=peer, device_id_type=MESH)

    for load in fetches:
        load.wait()
    for a, ref in enumerate((tok_in, grad_in)):
        value = ref[...].astype(F32)
        for q in range(parts // 2):
            at = (a * (parts // 2) + q) * rows
            packed[pl.ds(at, rows), :] = value[:, q * LANES : (q + 1) * LANES]
    blocks[odd, 0, here] = packed[...].astype(BF16)

    total_rows = n * block
    v = iota((1, total_rows), 1)
    b = lax.div(v, block)
    q = lax.div(v - b * block, rows)
    to = q * (n * rows) + b * rows + (v - b * block - q * rows)
    regroup = ones_where(iota((total_rows, total_rows), 0) == to)

    pl.semaphore_wait(barrier, len(peers))

    own = blocks.at[odd, 0, here]
    for k in near_first(n)[::-1]:
        copy = send(own, own, s_own.at[k], r_blk.at[odd, 0, here], at_own(k))
        copy.start()
        sends.append(copy)
    for k in near_first(n):
        copy = send(own, blocks.at[odd, k, here], s_blk.at[odd, k, 0], r_blk.at[odd, k, here], at_cross(k))
        copy.start()
        sends.append(copy)

    for load in loads:
        load.wait()
    for first in range(0, 3 * hidden, LANES):
        size = min(LANES, 3 * hidden - first)
        w_turned[:, pl.ds(first, size)] = w_all[pl.ds(first, size), :].T

    same, differ = spaced(n, 0), spaced(n, 1)

    def relay(axis, offset, s):
        place = lax.div(step(pick(x, z, axis), offset), 2)
        arrived(blocks.at[axis, 0, place], r_blk.at[axis, 0, place])
        for k in near_first(n):
            to_x, to_z = at_x(step(x, k))[1], at_z(step(z, k))[1]
            copy = send(
                blocks.at[axis, 0, place], blocks.at[axis, k, place],
                s_blk.at[axis, k, s], r_blk.at[axis, k, place], (row, pick(to_z, to_x, axis)),
            )
            copy.start()
            sends.append(copy)

    for s in range(half):
        relay(1 - odd, differ[s], s)
        if s + 1 < half:
            relay(odd, same[s + 1], s + 1)

    def partial(pairs):
        for k, _ in pairs:

            @pl.when(k != 0)
            def _(k=k):
                for axis in range(2):
                    for i in range(half):
                        arrived(blocks.at[axis, k, i], r_blk.at[axis, k, i])

        held = [
            jnp.concatenate([blocks[axis, k].reshape(half * block, LANES) for axis in range(2)], axis=0)
            for k, _ in pairs
        ]
        rows_of = plain(regroup, jnp.concatenate(held, axis=1)).astype(BF16)
        toks, grads = [], []
        for at, (_, o) in enumerate(pairs):
            lanes = rows_of[:, at * LANES : (at + 1) * LANES]
            cut = [lanes[q * group : (q + 1) * group] for q in range(parts)]
            toks.append(jnp.concatenate(cut[: parts // 2], axis=1))
            grads.append(jnp.concatenate(cut[parts // 2 :], axis=1))
            tok_full[o] = toks[-1]
            grad_full[o] = grads[-1]
        sums = plain(jnp.concatenate(toks, axis=0), w_turned[:, pl.ds(0, two)])
        backs = plain(jnp.concatenate(grads, axis=0), w_turned[:, pl.ds(two, hidden)])
        return jnp.concatenate([sums, backs], axis=1)

    batch = max(half // 2, 1)
    for m in range(0, half, batch):
        spots = range(m, m + batch)
        pair_src[m // batch] = partial([kept(i, 1 - core) for i in spots])
        copy = send(pair_src.at[m // batch], pair_dst.at[m // batch], s_pair.at[m], r_pair.at[m], pair)
        copy.start()
        sends.append(copy)
        part = partial([kept(i, core) for i in spots])
        copy.wait_recv()
        sums = part + pair_dst[m // batch]
        for at, i in enumerate(spots):
            _, g = kept(i, core)
            total = sums[at * group : (at + 1) * group]
            y_src[i] = total.astype(BF16)
            copy = send(y_src.at[i], y_dst.at[y], s_y.at[i], r_y.at[y], at_y(g))
            y_copies.append((g == y, copy))

            @pl.when(g != y)
            def _(copy=copy):
                copy.start()

            @pl.when(g == y)
            def _(total=total):
                own_sum[...] = total

    hid_order = near_first(n)
    direct = hid_order

    def handed_drain(lists):
        for ref, s_out, s_pass, r in lists:

            @pl.when(mine(y))
            def _(ref=ref, s_out=s_out, r=r):
                for copy in from_owner(ref, s_out, r):
                    copy.wait_send()

            for k in range(n):
                copy = to_pair(ref, s_pass, r, k)
                pl.when(mine(step(y, k)))(copy.wait_send)

    def from_owner(ref, s, r):
        return [send(ref.at[y], ref.at[y], s.at[k], r.at[y], at_y(step(y, k))) for k in direct]

    def to_pair(ref, s, r, k):
        g = step(y, k)
        return send(ref.at[g], ref.at[g], s.at[k], r.at[g], pair)

    def hand_on(ref, s, r, k):
        g = step(y, k)

        @pl.when(mine(g))
        def _():
            if k:
                arrived(ref.at[g], r.at[g])
            to_pair(ref, s, r, k).start()

    def handed(ref, r, k):
        g = step(y, k)
        pl.when(jnp.logical_not(mine(g)))(lambda: arrived(ref.at[g], r.at[g]))

    @pl.when(mine(y))
    def _():
        all_sums = own_sum[...]
        for k in hid_order:
            g = step(y, k)
            arrived(y_dst.at[g], r_y.at[g])
            all_sums = all_sums + y_dst[g].astype(F32)
        gate_sum, up_sum, back_sum = all_sums[:, :hidden], all_sums[:, hidden:two], all_sums[:, two:]
        sigmoid_gate = 1.0 / (1.0 + jnp.exp(-gate_sum))
        activated = gate_sum * sigmoid_gate
        slope = sigmoid_gate * (1.0 + gate_sum * (1.0 - sigmoid_gate))
        grads = jnp.concatenate([back_sum * up_sum * slope, back_sum * activated], axis=1)
        hid_g[y] = grads.astype(BF16)
        for copy in from_owner(hid_g, s_hid, r_hid):
            copy.start()
        hid_h[y] = (activated * up_sum).astype(BF16)

    def hidden_out():
        @pl.when(mine(y))
        def _():
            for copy in from_owner(hid_h, s_hidh, r_hidh):
                copy.start()

    def apart_for(count):
        i, j = iota((2 * room * count, 1), 0), iota((1, group * count), 1)
        block_of = lax.div(j, side)
        return ones_where(i == block_of * room + j - block_of * side)

    offsets = [0] + hid_order
    middle = n // 2 + 1
    for near in (offsets[:middle], offsets[middle:]):
        for k in near:
            hand_on(hid_g, s_fwd, r_hid, k)
        for k in near:
            handed(hid_g, r_hid, k)
        if not near:
            hidden_out()
            continue
        if near[0]:
            hidden_out()
        grads = jnp.concatenate([hid_g[step(y, k)] for k in near], axis=0)
        part = plain(grads, w_all[pl.ds(0, two), :]).astype(BF16)
        part = plain(apart_for(len(near)), part).astype(BF16)
        for at, k in enumerate(near):
            g = distance(step(y, k))
            home = g == 0
            for axis, a, place in ((0, z, at_z), (1, x, at_x)):
                device = place(step(a, n - g))
                first = (2 * at + axis) * room
                piece = part[first : first + room]
                d_src[axis, g] = piece
                copy = send(d_src.at[axis, g], d_dst.at[axis, g], s_d.at[axis, g], r_d.at[axis, g], device)
                d_copies.append((home, copy))

                @pl.when(jnp.logical_not(home))
                def _(copy=copy):
                    copy.start()

                @pl.when(home)
                def _(axis=axis, piece=piece):
                    d_dst[axis, 0] = piece

    tok_all = tok_full[...].reshape(n * group, width)
    grads_all = hid_g[...].reshape(n * group, two)
    gg_out[...] = down(grads_all[:, :hidden], tok_all).astype(BF16)
    gu_out[...] = down(grads_all[:, hidden:], tok_all).astype(BF16)

    i, j = iota((half * PAD, room), 0), iota((half * PAD, room), 1)
    low = i & (PAD - 1)
    spread = ones_where((low < rows) & (j == (i >> 3) * rows + low))
    spread = jnp.concatenate([spread] * n, axis=1)
    for axis in range(2):
        for k in range(1, n):
            arrived(d_dst.at[axis, k], r_d.at[axis, k])
        summed = plain(spread, d_dst[axis].reshape(n * room, width))
        e_src[axis] = summed.reshape(half, PAD, width)
        line, cross = (z, x) if axis else (x, z)
        for i in range(half):
            place = 2 * i + lax.rem(cross + axis, 2)
            device = at_z(place) if axis else at_x(place)
            is_self = place == line
            copy = send(e_src.at[axis, i], e_dst.at[line], s_e.at[axis, i], r_e.at[line], device)
            e_copies.append((is_self, copy))

            @pl.when(jnp.logical_not(is_self))
            def _(copy=copy):
                copy.start()

            @pl.when(is_self)
            def _(axis=axis, i=i, line=line):
                e_dst[line] = e_src[axis, i]

    for k in offsets:
        hand_on(hid_h, s_fwdh, r_hidh, k)
    for k in offsets:
        handed(hid_h, r_hidh, k)

    grad_all = grad_full[...].reshape(n * group, width)
    hidden_all = hid_h[...].reshape(n * group, hidden)
    gd_out[...] = down(hidden_all, grad_all).astype(BF16)

    for k in range(1, n):
        g = step(spot, k)
        arrived(e_dst.at[g], r_e.at[g])
    gtok_ref[...] = jnp.sum(e_dst[...], axis=0)[:rows].astype(BF16)

    drain()
    handed_drain(((hid_g, s_hid, s_fwd, r_hid), (hid_h, s_hidh, s_fwdh, r_hidh)))


def put_out(*refs):
    count = (len(refs) - 1) // 2
    copies = [pltpu.make_async_copy(refs[i], refs[count + i], refs[-1].at[i]) for i in range(count)]
    for copy in copies:
        copy.start()
    for copy in copies:
        copy.wait()


def shards(n, tokens, grad_out, gate_weight, up_weight, down_weight):
    rows, width = tokens.shape
    hidden = down_weight.shape[0]
    two, half = 2 * hidden, n // 2
    side = rows * half
    batch = max(half // 2, 1)
    group = 2 * side
    room = -(-side // PAD) * PAD
    block = rows * 2 * width // LANES
    dma = pltpu.SemaphoreType.DMA
    out = jax.ShapeDtypeStruct((hidden, width), BF16)
    outs = (jax.ShapeDtypeStruct((rows, width), BF16), out, out, out)
    vmem = pl.BlockSpec(memory_space=pltpu.VMEM)
    hbm = pl.BlockSpec(memory_space=pltpu.HBM)
    results = pl.pallas_call(
        functools.partial(kernel, n),
        out_shape=outs,
        in_specs=[hbm] * 5,
        out_specs=(vmem,) * 4,
        scratch_shapes=[
            pltpu.VMEM((rows, width), BF16),
            pltpu.VMEM((rows, width), BF16),
            pltpu.VMEM((block, LANES), F32),
            pltpu.VMEM((3 * hidden, width), BF16),
            pltpu.VMEM((width, 3 * hidden), BF16),
            pltpu.VMEM((2, n, half, block, LANES), BF16),
            pltpu.VMEM((n, group, width), BF16),
            pltpu.VMEM((n, group, width), BF16),
            pltpu.VMEM((half // batch, batch * group, 3 * hidden), F32),
            pltpu.VMEM((half // batch, batch * group, 3 * hidden), F32),
            pltpu.VMEM((group, 3 * hidden), F32),
            pltpu.VMEM((half, group, 3 * hidden), BF16),
            pltpu.VMEM((n, group, 3 * hidden), BF16),
            pltpu.VMEM((n, group, two), BF16),
            pltpu.VMEM((n, group, hidden), BF16),
            pltpu.VMEM((2, n, room, width), BF16),
            pltpu.VMEM((2, n, room, width), BF16),
            pltpu.VMEM((2, half, PAD, width), F32),
            pltpu.VMEM((n, PAD, width), F32),
            dma((5,)),
            dma((n,)), dma((2, n, half)), dma((2, n, half)),
            dma((half,)), dma((half,)), dma((half,)), dma((n,)),
            dma((n,)), dma((n,)), dma((n,)), dma((n,)), dma((n,)), dma((n,)),
            dma((2, n)), dma((2, n)), dma((2, half)), dma((n,)),
        ],
        compiler_params=pltpu.CompilerParams(collective_id=0, has_side_effects=True, vmem_limit_bytes=32 * MIB),
        name="block",
    )(*[pltpu.with_memory_space_constraint(v, pltpu.HBM) for v in (tokens, grad_out, gate_weight.T, up_weight.T, down_weight)])
    grad_tokens, gate_t, up_t, grad_down = pl.pallas_call(
        put_out,
        out_shape=outs,
        in_specs=[vmem] * 4,
        out_specs=(hbm,) * 4,
        scratch_shapes=[dma((4,))],
        compiler_params=pltpu.CompilerParams(vmem_limit_bytes=16 * MIB),
        name="put_out",
    )(*results)
    return grad_tokens, gate_t.T, up_t.T, grad_down


def solution(mesh):
    n = mesh.shape["row"] // 2
    placed = (P("col", "row"), P("col", "row"), P("row", "col"), P("row", "col"), P("col", "row"))
    return jax.shard_map(
        functools.partial(shards, n),
        mesh=mesh,
        in_specs=placed,
        out_specs=(P("col", "row"), P("row", "col"), P("row", "col"), P("col", "row")),
        check_vma=False,
    )
```

```python
import functools

import jax
import jax.numpy as jnp
from jax import lax
from jax.experimental import pallas as pl
from jax.experimental.pallas import tpu as pltpu
from jax.sharding import PartitionSpec as P

MESH = pl.DeviceIdType.MESH
BF16 = jnp.bfloat16
F32 = jnp.float32
PAD = 8
LANES = 128
MIB = 1024 * 1024


def near_first(n):
    order = []
    for k in range(1, n // 2 + 1):
        order.append(k)
        if n - k != k:
            order.append(n - k)
    return order


def spaced(n, odd):
    return [0] * (1 - odd) + [k for k in near_first(n) if k % 2 == odd]


def groups_of(n):
    half = n // 2
    ks = ([(n - m) % n for m in range(half)], [m + 1 for m in range(half)])
    if n == 8:
        owners = ([0, 4, 1, 5], [2, 6, 3, 7])
    else:
        owners = (list(range(half)), list(range(half, n)))
    return ks, owners


def down(a, b):
    return lax.dot_general(a, b, (((0,), (0,)), ((), ())), preferred_element_type=F32)


def plain(a, b):
    return lax.dot_general(a, b, (((1,), (0,)), ((), ())), preferred_element_type=F32)


def iota(shape, dim):
    return lax.broadcasted_iota(jnp.int32, shape, dim)


def ones_where(mask):
    return mask.astype(F32).astype(BF16)


def kernel(
    n,
    tok_ref, grad_ref, wg_ref, wu_ref, wd_ref,
    gtok_ref, gg_out, gu_out, gd_out,
    tok_in, grad_in, packed, w_all, w_turned, blocks, tok_full, grad_full,
    pair_src, pair_dst, own_sum, y_src, y_dst, hid_g, hid_h, d_src, d_dst, e_src, e_dst,
    load_sem, s_own, s_blk, r_blk, s_pair, r_pair, s_y, r_y, s_hid, r_hid, s_fwd, s_hidh, r_hidh, s_fwdh, s_d, r_d, s_e, r_e,
):
    rows, width = tok_in.shape
    hidden = wd_ref.shape[0]
    two = 2 * hidden
    half = n // 2
    side = rows * half
    group = 2 * side
    room = d_src.shape[2]
    parts = 2 * width // LANES
    block = rows * parts

    row, col = lax.axis_index("row"), lax.axis_index("col")
    y, core = lax.div(row, 2), lax.rem(row, 2)
    z, x = lax.div(col, n), lax.rem(col, n)
    odd = lax.rem(z + x, 2)
    pair = (row + 1 - 2 * core, col)
    spot = x + odd * (z - x)
    here = lax.div(spot, 2)

    def step(a, k):
        return lax.rem(a + k, n)

    def at_x(k):
        return (row, z * n + k)

    def at_z(k):
        return (row, k * n + x)

    def at_y(k):
        return (2 * k + core, col)

    def at_own(k):
        other = step(spot, k)
        return (row, (z * n + other) * (1 - odd) + (other * n + x) * odd)

    def at_cross(k):
        return (row, (z * n + step(x, k)) * odd + (step(z, k) * n + x) * (1 - odd))

    def send(src, dst, s, r, device):
        return pltpu.make_async_remote_copy(
            src_ref=src, dst_ref=dst, send_sem=s, recv_sem=r, device_id=device, device_id_type=MESH
        )

    def arrived(dst, sem):
        send(dst, dst, sem, sem, pair).wait_recv()

    ks, owners = groups_of(n)

    def pick(first, second, who):
        return first * (1 - who) + second * who

    def kept(m, who):
        return pick(ks[0][m], ks[1][m], who), pick(owners[0][m], owners[1][m], who)

    def mine(o):
        found = [o == pick(owners[0][m], owners[1][m], core) for m in range(half)]
        return functools.reduce(jnp.logical_or, found)

    def distance(o):
        return sum(jnp.where(o == owners[w][m], ks[w][m], 0) for w in range(2) for m in range(half))

    sends = []
    y_copies, d_copies, e_copies = [], [], []

    def drain():
        for copy in sends:
            copy.wait_send()
        for clash, copy in y_copies + d_copies + e_copies:

            @pl.when(jnp.logical_not(clash))
            def _(copy=copy):
                copy.wait_send()

    fetches = [
        pltpu.make_async_copy(tok_ref, tok_in, load_sem.at[0]),
        pltpu.make_async_copy(grad_ref, grad_in, load_sem.at[1]),
    ]
    loads = [
        pltpu.make_async_copy(wg_ref, w_all.at[pl.ds(0, hidden)], load_sem.at[2]),
        pltpu.make_async_copy(wu_ref, w_all.at[pl.ds(hidden, hidden)], load_sem.at[3]),
        pltpu.make_async_copy(wd_ref, w_all.at[pl.ds(two, hidden)], load_sem.at[4]),
    ]
    for load in fetches + loads:
        load.start()

    barrier = pltpu.get_barrier_semaphore()
    peers = [at(step(a, k)) for at, a in ((at_x, x), (at_z, z), (at_y, y)) for k in range(1, n)] + [pair]
    for peer in peers:
        pl.semaphore_signal(barrier, inc=1, device_id=peer, device_id_type=MESH)

    for load in fetches:
        load.wait()
    for a, ref in enumerate((tok_in, grad_in)):
        value = ref[...].astype(F32)
        for q in range(parts // 2):
            at = (a * (parts // 2) + q) * rows
            packed[pl.ds(at, rows), :] = value[:, q * LANES : (q + 1) * LANES]
    blocks[odd, 0, here] = packed[...].astype(BF16)

    total_rows = n * block
    v = iota((1, total_rows), 1)
    b = lax.div(v, block)
    q = lax.div(v - b * block, rows)
    to = q * (n * rows) + b * rows + (v - b * block - q * rows)
    regroup = ones_where(iota((total_rows, total_rows), 0) == to)

    pl.semaphore_wait(barrier, len(peers))

    own = blocks.at[odd, 0, here]
    for k in near_first(n)[::-1]:
        copy = send(own, own, s_own.at[k], r_blk.at[odd, 0, here], at_own(k))
        copy.start()
        sends.append(copy)
    for k in near_first(n):
        copy = send(own, blocks.at[odd, k, here], s_blk.at[odd, k, 0], r_blk.at[odd, k, here], at_cross(k))
        copy.start()
        sends.append(copy)

    for load in loads:
        load.wait()
    for first in range(0, 3 * hidden, LANES):
        size = min(LANES, 3 * hidden - first)
        w_turned[:, pl.ds(first, size)] = w_all[pl.ds(first, size), :].T

    same, differ = spaced(n, 0), spaced(n, 1)

    def relay(axis, offset, s):
        place = lax.div(step(pick(x, z, axis), offset), 2)
        arrived(blocks.at[axis, 0, place], r_blk.at[axis, 0, place])
        for k in near_first(n):
            to_x, to_z = at_x(step(x, k))[1], at_z(step(z, k))[1]
            copy = send(
                blocks.at[axis, 0, place], blocks.at[axis, k, place],
                s_blk.at[axis, k, s], r_blk.at[axis, k, place], (row, pick(to_z, to_x, axis)),
            )
            copy.start()
            sends.append(copy)

    waits = [(min(k, n - k), 1, s, k) for s, k in enumerate(differ)]
    waits += [(min(k, n - k), 0, s, k) for s, k in enumerate(same) if s]
    for _, crossed, s, k in sorted(waits):
        relay(1 - odd if crossed else odd, k, s)

    def partial(pairs):
        for k, _ in pairs:

            @pl.when(k != 0)
            def _(k=k):
                for axis in range(2):
                    for i in range(half):
                        arrived(blocks.at[axis, k, i], r_blk.at[axis, k, i])

        held = [
            jnp.concatenate([blocks[axis, k].reshape(half * block, LANES) for axis in range(2)], axis=0)
            for k, _ in pairs
        ]
        rows_of = plain(regroup, jnp.concatenate(held, axis=1)).astype(BF16)
        toks, grads = [], []
        for at, (_, o) in enumerate(pairs):
            lanes = rows_of[:, at * LANES : (at + 1) * LANES]
            cut = [lanes[q * group : (q + 1) * group] for q in range(parts)]
            toks.append(jnp.concatenate(cut[: parts // 2], axis=1))
            grads.append(jnp.concatenate(cut[parts // 2 :], axis=1))
            tok_full[o] = toks[-1]
            grad_full[o] = grads[-1]
        sums = plain(jnp.concatenate(toks, axis=0), w_turned[:, pl.ds(0, two)])
        backs = plain(jnp.concatenate(grads, axis=0), w_turned[:, pl.ds(two, hidden)])
        return jnp.concatenate([sums, backs], axis=1)

    batch = max(half // 2, 1)
    for m in range(0, half, batch):
        spots = range(m, m + batch)
        pair_src[m // batch] = partial([kept(i, 1 - core) for i in spots])
        copy = send(pair_src.at[m // batch], pair_dst.at[m // batch], s_pair.at[m], r_pair.at[m], pair)
        copy.start()
        sends.append(copy)
        part = partial([kept(i, core) for i in spots])
        copy.wait_recv()
        sums = part + pair_dst[m // batch]
        for at, i in enumerate(spots):
            _, g = kept(i, core)
            total = sums[at * group : (at + 1) * group]
            y_src[i] = total.astype(BF16)
            copy = send(y_src.at[i], y_dst.at[y], s_y.at[i], r_y.at[y], at_y(g))
            y_copies.append((g == y, copy))

            @pl.when(g != y)
            def _(copy=copy):
                copy.start()

            @pl.when(g == y)
            def _(total=total):
                own_sum[...] = total

    hid_order = near_first(n)
    direct = hid_order

    def handed_drain(lists):
        for ref, s_out, s_pass, r in lists:

            @pl.when(mine(y))
            def _(ref=ref, s_out=s_out, r=r):
                for copy in from_owner(ref, s_out, r):
                    copy.wait_send()

            for k in range(n):
                copy = to_pair(ref, s_pass, r, k)
                pl.when(mine(step(y, k)))(copy.wait_send)

    def from_owner(ref, s, r):
        return [send(ref.at[y], ref.at[y], s.at[k], r.at[y], at_y(step(y, k))) for k in direct]

    def to_pair(ref, s, r, k):
        g = step(y, k)
        return send(ref.at[g], ref.at[g], s.at[k], r.at[g], pair)

    def hand_on(ref, s, r, k):
        g = step(y, k)

        @pl.when(mine(g))
        def _():
            if k:
                arrived(ref.at[g], r.at[g])
            to_pair(ref, s, r, k).start()

    def handed(ref, r, k):
        g = step(y, k)
        pl.when(jnp.logical_not(mine(g)))(lambda: arrived(ref.at[g], r.at[g]))

    @pl.when(mine(y))
    def _():
        all_sums = own_sum[...]
        for k in hid_order:
            g = step(y, k)
            arrived(y_dst.at[g], r_y.at[g])
            all_sums = all_sums + y_dst[g].astype(F32)
        gate_sum, up_sum, back_sum = all_sums[:, :hidden], all_sums[:, hidden:two], all_sums[:, two:]
        sigmoid_gate = 1.0 / (1.0 + jnp.exp(-gate_sum))
        activated = gate_sum * sigmoid_gate
        slope = sigmoid_gate * (1.0 + gate_sum * (1.0 - sigmoid_gate))
        grads = jnp.concatenate([back_sum * up_sum * slope, back_sum * activated], axis=1)
        hid_g[y] = grads.astype(BF16)
        for copy in from_owner(hid_g, s_hid, r_hid):
            copy.start()
        hid_h[y] = (activated * up_sum).astype(BF16)

    def hidden_out():
        @pl.when(mine(y))
        def _():
            for copy in from_owner(hid_h, s_hidh, r_hidh):
                copy.start()

    def apart_for(count):
        i, j = iota((2 * room * count, 1), 0), iota((1, group * count), 1)
        block_of = lax.div(j, side)
        return ones_where(i == block_of * room + j - block_of * side)

    offsets = [0] + hid_order
    middle = n // 2 + 1
    for near in (offsets[:middle], offsets[middle:]):
        for k in near:
            hand_on(hid_g, s_fwd, r_hid, k)
        for k in near:
            handed(hid_g, r_hid, k)
        if not near:
            hidden_out()
            continue
        if near[0]:
            hidden_out()
        grads = jnp.concatenate([hid_g[step(y, k)] for k in near], axis=0)
        part = plain(grads, w_all[pl.ds(0, two), :]).astype(BF16)
        part = plain(apart_for(len(near)), part).astype(BF16)
        for at, k in enumerate(near):
            g = distance(step(y, k))
            home = g == 0
            for axis, a, place in ((0, z, at_z), (1, x, at_x)):
                device = place(step(a, n - g))
                first = (2 * at + axis) * room
                piece = part[first : first + room]
                d_src[axis, g] = piece
                copy = send(d_src.at[axis, g], d_dst.at[axis, g], s_d.at[axis, g], r_d.at[axis, g], device)
                d_copies.append((home, copy))

                @pl.when(jnp.logical_not(home))
                def _(copy=copy):
                    copy.start()

                @pl.when(home)
                def _(axis=axis, piece=piece):
                    d_dst[axis, 0] = piece

    tok_all = tok_full[...].reshape(n * group, width)
    grads_all = hid_g[...].reshape(n * group, two)
    gg_out[...] = down(grads_all[:, :hidden], tok_all).astype(BF16)
    gu_out[...] = down(grads_all[:, hidden:], tok_all).astype(BF16)

    i, j = iota((half * PAD, room), 0), iota((half * PAD, room), 1)
    low = i & (PAD - 1)
    spread = ones_where((low < rows) & (j == (i >> 3) * rows + low))
    spread = jnp.concatenate([spread] * n, axis=1)
    for axis in range(2):
        for k in range(1, n):
            arrived(d_dst.at[axis, k], r_d.at[axis, k])
        summed = plain(spread, d_dst[axis].reshape(n * room, width))
        e_src[axis] = summed.reshape(half, PAD, width)
        line, cross = (z, x) if axis else (x, z)
        for i in range(half):
            place = 2 * i + lax.rem(cross + axis, 2)
            device = at_z(place) if axis else at_x(place)
            is_self = place == line
            copy = send(e_src.at[axis, i], e_dst.at[line], s_e.at[axis, i], r_e.at[line], device)
            e_copies.append((is_self, copy))

            @pl.when(jnp.logical_not(is_self))
            def _(copy=copy):
                copy.start()

            @pl.when(is_self)
            def _(axis=axis, i=i, line=line):
                e_dst[line] = e_src[axis, i]

    for k in offsets:
        hand_on(hid_h, s_fwdh, r_hidh, k)
    for k in offsets:
        handed(hid_h, r_hidh, k)

    grad_all = grad_full[...].reshape(n * group, width)
    hidden_all = hid_h[...].reshape(n * group, hidden)
    gd_out[...] = down(hidden_all, grad_all).astype(BF16)

    for k in range(1, n):
        g = step(spot, k)
        arrived(e_dst.at[g], r_e.at[g])
    gtok_ref[...] = jnp.sum(e_dst[...], axis=0)[:rows].astype(BF16)

    drain()
    handed_drain(((hid_g, s_hid, s_fwd, r_hid), (hid_h, s_hidh, s_fwdh, r_hidh)))


def put_out(*refs):
    count = (len(refs) - 1) // 2
    copies = [pltpu.make_async_copy(refs[i], refs[count + i], refs[-1].at[i]) for i in range(count)]
    for copy in copies:
        copy.start()
    for copy in copies:
        copy.wait()


def shards(n, tokens, grad_out, gate_weight, up_weight, down_weight):
    rows, width = tokens.shape
    hidden = down_weight.shape[0]
    two, half = 2 * hidden, n // 2
    side = rows * half
    batch = max(half // 2, 1)
    group = 2 * side
    room = -(-side // PAD) * PAD
    block = rows * 2 * width // LANES
    dma = pltpu.SemaphoreType.DMA
    out = jax.ShapeDtypeStruct((hidden, width), BF16)
    outs = (jax.ShapeDtypeStruct((rows, width), BF16), out, out, out)
    vmem = pl.BlockSpec(memory_space=pltpu.VMEM)
    hbm = pl.BlockSpec(memory_space=pltpu.HBM)
    results = pl.pallas_call(
        functools.partial(kernel, n),
        out_shape=outs,
        in_specs=[hbm] * 5,
        out_specs=(vmem,) * 4,
        scratch_shapes=[
            pltpu.VMEM((rows, width), BF16),
            pltpu.VMEM((rows, width), BF16),
            pltpu.VMEM((block, LANES), F32),
            pltpu.VMEM((3 * hidden, width), BF16),
            pltpu.VMEM((width, 3 * hidden), BF16),
            pltpu.VMEM((2, n, half, block, LANES), BF16),
            pltpu.VMEM((n, group, width), BF16),
            pltpu.VMEM((n, group, width), BF16),
            pltpu.VMEM((half // batch, batch * group, 3 * hidden), F32),
            pltpu.VMEM((half // batch, batch * group, 3 * hidden), F32),
            pltpu.VMEM((group, 3 * hidden), F32),
            pltpu.VMEM((half, group, 3 * hidden), BF16),
            pltpu.VMEM((n, group, 3 * hidden), BF16),
            pltpu.VMEM((n, group, two), BF16),
            pltpu.VMEM((n, group, hidden), BF16),
            pltpu.VMEM((2, n, room, width), BF16),
            pltpu.VMEM((2, n, room, width), BF16),
            pltpu.VMEM((2, half, PAD, width), F32),
            pltpu.VMEM((n, PAD, width), F32),
            dma((5,)),
            dma((n,)), dma((2, n, half)), dma((2, n, half)),
            dma((half,)), dma((half,)), dma((half,)), dma((n,)),
            dma((n,)), dma((n,)), dma((n,)), dma((n,)), dma((n,)), dma((n,)),
            dma((2, n)), dma((2, n)), dma((2, half)), dma((n,)),
        ],
        compiler_params=pltpu.CompilerParams(collective_id=0, has_side_effects=True, vmem_limit_bytes=32 * MIB),
        name="block",
    )(*[pltpu.with_memory_space_constraint(v, pltpu.HBM) for v in (tokens, grad_out, gate_weight.T, up_weight.T, down_weight)])
    grad_tokens, gate_t, up_t, grad_down = pl.pallas_call(
        put_out,
        out_shape=outs,
        in_specs=[vmem] * 4,
        out_specs=(hbm,) * 4,
        scratch_shapes=[dma((4,))],
        compiler_params=pltpu.CompilerParams(vmem_limit_bytes=16 * MIB),
        name="put_out",
    )(*results)
    return grad_tokens, gate_t.T, up_t.T, grad_down


def solution(mesh):
    n = mesh.shape["row"] // 2
    placed = (P("col", "row"), P("col", "row"), P("row", "col"), P("row", "col"), P("col", "row"))
    return jax.shard_map(
        functools.partial(shards, n),
        mesh=mesh,
        in_specs=placed,
        out_specs=(P("col", "row"), P("row", "col"), P("row", "col"), P("col", "row")),
        check_vma=False,
    )
```
